32 devices in a mesh: seq: 8 (over z, y), head: 4 (over x, core).
Axes of the slice: x: 2, y: 2, z: 4, core: 2. Of those that a mesh axis runs over, the one named last changes fastest.
Arguments:
- queries: bfloat16 [2048, 2048], P(('seq', 'head')), may hold values from -200 to 200
- keys: bfloat16 [2048, 2048], P(('seq', 'head')), may hold values from -15 to 15
- values: bfloat16 [2048, 2048], P(('seq', 'head')), may hold values from -6 to 6
- random_blocks: int32 [32, 16, 3], P('seq', 'head'), may hold values from 0 to 31, as said below
- global_blocks: int32 [2], replicated, may hold values from 0 to 31, as said below
Outputs:
- attention: float32 [2048, 2048], P('seq', 'head')
The draws below stay inside these ranges and needn't reach their ends.
Inputs may be any that keep to these rules, and one draw needn't show every extreme that they name: `random_blocks`: over the 4 query blocks and 4 heads of one device (one index of seq and one of head), at most 9 entries name blocks of any one shard of 4 consecutive blocks; in every draw some device names exactly 9 blocks of one shard. Entries may repeat and may fall on the window or on a global block. `global_blocks`: two different block numbers; one of them is 31.
All inputs are finite; a program needn't handle non-finite values.
Results may differ from the reference program's by a relative error of at most 0.0023.
Values may be sent and summed in bfloat16 or wider, within the bound.
A program may use at most 128 MiB of HBM per device.

```python
import math
import jax
import jax.numpy as jnp
from jax import lax

HEADS = 16
HEAD_DIM = 128
BLK = 64
RAND = 3
GLOB = 2
BLK_DEV = 4
HEADS_DEV = 4
NB = 32
TOKENS = 2048
CAP = 9


def draw_pair(key):
    base_key = jax.random.fold_in(key, 101)
    query_key, key_key = jax.random.split(base_key, 2)
    dims = (TOKENS, HEADS * HEAD_DIM)
    query_draw = 2.0 * jnp.clip(jax.random.normal(query_key, dims, jnp.float32), -6.0, 6.0)
    key_draw = jnp.clip(jax.random.normal(key_key, dims, jnp.float32), -6.0, 6.0)
    return (query_draw, key_draw)


def draw_queries(key, part):
    return draw_pair(key)[0].astype(jnp.bfloat16)


def draw_keys(key, part):
    return draw_pair(key)[1].astype(jnp.bfloat16)


def draw_random_blocks(key, part):
    base_key = jax.random.fold_in(key, 202)
    seq_count = NB // BLK_DEV
    head_groups = HEADS // HEADS_DEV
    per_device = BLK_DEV * HEADS_DEV * RAND

    def one_device(device_key):
        perm_key, favor_key, order_key, block_key = jax.random.split(device_key, 4)
        owners = jnp.tile(jnp.arange(seq_count, dtype=jnp.int32), CAP)
        favored = jax.random.randint(favor_key, (), 0, seq_count)
        shuffled = jax.random.permutation(perm_key, seq_count * CAP).astype(jnp.int32)
        ranking = jnp.where(owners == favored, -1, shuffled)
        chosen = owners[jnp.argsort(ranking, stable=True)][:per_device]
        chosen = chosen[jax.random.permutation(order_key, per_device)]
        offsets = jax.random.randint(block_key, (per_device,), 0, BLK_DEV)
        return (chosen * BLK_DEV + offsets).astype(jnp.int32).reshape(BLK_DEV, HEADS_DEV, RAND)
    device_keys = jax.random.split(base_key, seq_count * head_groups)
    drawn = jax.vmap(one_device)(device_keys)
    drawn = drawn.reshape(seq_count, head_groups, BLK_DEV, HEADS_DEV, RAND).transpose(0, 2, 1, 3, 4)
    return drawn.reshape(NB, HEADS, RAND)


def draw_global_blocks(key, part):
    base_key = jax.random.fold_in(key, 303)
    other_key, place_key = jax.random.split(base_key, 2)
    other = jax.random.randint(other_key, (), 0, NB - 1).astype(jnp.int32)
    last = jnp.array(NB - 1, jnp.int32)
    place = jax.random.randint(place_key, (), 0, 2)
    first_entry = jnp.where(place == 0, last, other)
    second_entry = jnp.where(place == 0, other, last)
    return jnp.stack([first_entry, second_entry]).astype(jnp.int32)


def level_of(rng, extent, cuts, least, high):
    loudness, own = 1.0, jax.random.fold_in(rng, 6)
    for dim, shards_of in cuts:
        steps = jnp.exp(jax.random.uniform(jax.random.fold_in(own, dim), (shards_of,), jnp.float32, least / len(cuts), high / len(cuts)))
        loudness = loudness * jnp.repeat(steps, extent[dim] // shards_of).reshape([-1 if axis == dim else 1 for axis in range(len(extent))])
    return loudness


def scatter_about(key, extent, deviation, most, pieces=(), held_as=jnp.bfloat16):
    entries = deviation * jax.random.normal(key, extent, jnp.float32)
    if pieces:
        entries = entries * level_of(key, extent, pieces, -0.22, 0.18)
    return jnp.clip(entries, -most, most).astype(held_as)


def setup_inputs(seed: int = 0) -> dict:
    key_of = jax.random.split(jax.random.key(seed), 6)
    queries = draw_queries(jax.random.fold_in(key_of[5], 71), 0)
    keys = draw_keys(jax.random.fold_in(key_of[5], 71), 0)
    values = scatter_about(key_of[2], (TOKENS, HEADS * HEAD_DIM), 1.0, 6.0, ((0, 32),))
    random_blocks = draw_random_blocks(jax.random.fold_in(key_of[5], 71), 0)
    global_blocks = draw_global_blocks(jax.random.fold_in(key_of[5], 71), 0)
    return dict(queries=queries, keys=keys, values=values, random_blocks=random_blocks, global_blocks=global_blocks)


MASKED = -1e+30

def attend(scores, value_set):
    peaks = lax.optimization_barrier(jnp.max(scores, axis=-1, keepdims=True))
    powers = jnp.exp(scores - peaks)
    totals = lax.optimization_barrier(jnp.sum(powers, axis=-1, keepdims=True))
    weights = lax.optimization_barrier(powers.astype(jnp.bfloat16)).astype(jnp.float32)
    return jnp.einsum('hqk,hkd->hqd', weights, value_set.astype(jnp.float32)) / totals

def reference(queries, keys, values, random_blocks, global_blocks):
    score_scale = 1.0 / math.sqrt(HEAD_DIM)
    block_shape = (NB, BLK, HEADS, HEAD_DIM)
    query_blocks = queries.reshape(block_shape)
    key_blocks = keys.reshape(block_shape)
    value_blocks = values.reshape(block_shape)
    head_ids = jnp.arange(HEADS, dtype=jnp.int32)[:, None]

    def gather_blocks(source_table, block_id, rand_ids):
        near_ids = jnp.clip(block_id + jnp.arange(-1, 2, dtype=jnp.int32), 0, NB - 1)
        window = jnp.transpose(source_table[near_ids], (2, 0, 1, 3))
        global_part = jnp.transpose(source_table[global_blocks], (2, 0, 1, 3))
        random_part = source_table[rand_ids, :, head_ids, :]
        joined = jnp.concatenate([window, global_part, random_part], axis=1)
        return joined.reshape(HEADS, (3 + GLOB + RAND) * BLK, HEAD_DIM)

    def sparse_row(block_id):
        rand_ids = random_blocks[block_id]
        near_ids = block_id + jnp.arange(-1, 2, dtype=jnp.int32)
        in_range = (near_ids >= 0) & (near_ids < NB)
        keep_mask = jnp.concatenate([jnp.repeat(in_range, BLK), jnp.ones(((GLOB + RAND) * BLK,), dtype=bool)])
        key_set = gather_blocks(key_blocks, block_id, rand_ids).astype(jnp.float32)
        value_set = gather_blocks(value_blocks, block_id, rand_ids)
        query_set = jnp.transpose(query_blocks[block_id], (1, 0, 2)).astype(jnp.float32)
        scores = jnp.einsum('hqd,hkd->hqk', query_set, key_set) * score_scale
        scores = jnp.where(keep_mask[None, None, :], scores, MASKED)
        return attend(scores, value_set)
    sparse = lax.map(sparse_row, jnp.arange(NB, dtype=jnp.int32))
    sparse = jnp.transpose(sparse, (0, 2, 1, 3))
    global_query = query_blocks[global_blocks]
    flat_keys = keys.reshape(TOKENS, HEADS, HEAD_DIM)
    flat_values = values.reshape(TOKENS, HEADS, HEAD_DIM)

    def full_head(head_id):
        query_set = jnp.take(global_query, head_id, axis=2).reshape(GLOB * BLK, HEAD_DIM)
        key_set = jnp.take(flat_keys, head_id, axis=1)
        value_set = jnp.take(flat_values, head_id, axis=1)
        scores = jnp.dot(query_set, key_set.T, preferred_element_type=jnp.float32) * score_scale
        return attend(scores[None], value_set[None])[0]
    full_rows = lax.map(full_head, jnp.arange(HEADS, dtype=jnp.int32))
    full_rows = jnp.transpose(full_rows.reshape(HEADS, GLOB, BLK, HEAD_DIM), (1, 2, 0, 3))
    attention = sparse.at[global_blocks].set(full_rows)
    return attention.reshape(TOKENS, HEADS * HEAD_DIM)
```

```python
import functools
import math

import jax
import jax.numpy as jnp
from jax import lax
from jax.experimental import pallas as pl
from jax.experimental.pallas import tpu as pltpu
from jax.sharding import PartitionSpec as P

HEAD_DIM = 128
BLK = 64


MASKED = -1e30


def extended(block, sides, width):
    for axis, dim in sides:
        count = lax.axis_size(axis)
        forward = [(i, i + 1) for i in range(count - 1)]
        backward = [(target, source) for source, target in forward]
        low = lax.ppermute(
            lax.slice_in_dim(block, block.shape[dim] - width, None, axis=dim), axis, forward
        )
        high = lax.ppermute(lax.slice_in_dim(block, 0, width, axis=dim), axis, backward)
        block = jnp.concatenate([low, block, high], axis=dim)
    return block


def combined_all(value, axis, join):
    pieces = jax.tree.map(lambda part: lax.all_gather(part, axis), value)
    head = jax.tree.map(lambda part: part[0], pieces)
    tail = jax.tree.map(lambda part: part[1:], pieces)
    so_far, _ = lax.scan(lambda so_far, slab: (join(so_far, slab), None), head, tail)
    return so_far


def merge_parts(former, latter):
    peaks = jnp.maximum(former[0], latter[0])
    former_fade = jnp.exp(former[0] - peaks)
    latter_fade = jnp.exp(latter[0] - peaks)
    return (
        peaks,
        former[1] * former_fade + latter[1] * latter_fade,
        former[2] * former_fade[..., None] + latter[2] * latter_fade[..., None],
    )


def soft_parts(scores):
    peaks = jnp.max(scores, axis=(-2, -1))
    powers = jnp.exp(scores - peaks[..., None, None])
    return (peaks, jnp.sum(powers, axis=(-2, -1)), powers.astype(jnp.bfloat16))


def make_requests(rand_lists, seq_count, capacity):
    blk_dev, heads_dev, rand_count = rand_lists.shape
    flat_list = rand_lists.reshape(-1)
    owners = flat_list // blk_dev
    head_ids = jnp.broadcast_to(
        jnp.arange(heads_dev, dtype=jnp.int32)[None, :, None], rand_lists.shape
    ).reshape(-1)
    item_ids = flat_list % blk_dev * heads_dev + head_ids
    position = jnp.arange(flat_list.shape[0], dtype=jnp.int32)
    earlier = (owners[:, None] == owners[None, :]) & (position[None, :] < position[:, None])
    slot_ids = owners * capacity + jnp.sum(earlier.astype(jnp.int32), axis=1)
    requests = jnp.zeros((seq_count * capacity,), jnp.int32).at[slot_ids].set(item_ids)
    sources = jnp.zeros((seq_count * capacity,), jnp.int32).at[slot_ids].set(position)
    return (requests.reshape(seq_count, capacity), slot_ids, sources)


def exchanged(queries, keys, values, random_blocks, global_blocks):
    seq_count = lax.axis_size("seq")
    seq_index = lax.axis_index("seq")
    query_rows, key_rows, value_rows = (
        lax.all_to_all(queries, "head", split_axis=1, concat_axis=0, tiled=True),
        lax.all_to_all(keys, "head", split_axis=1, concat_axis=0, tiled=True),
        lax.all_to_all(values, "head", split_axis=1, concat_axis=0, tiled=True),
    )
    tokens = query_rows.shape[0]
    blk_dev = tokens // BLK
    heads_dev = query_rows.shape[1] // HEAD_DIM
    rand_count = random_blocks.shape[2]
    glob_count = global_blocks.shape[0]
    total_blocks = blk_dev * seq_count
    first_block = seq_index * blk_dev
    capacity = (blk_dev * heads_dev * rand_count * 3 // 2 + seq_count - 1) // seq_count
    score_scale = 1.0 / math.sqrt(HEAD_DIM)
    shape_four = (blk_dev, BLK, heads_dev, HEAD_DIM)
    query_four = query_rows.reshape(shape_four)
    key_four = key_rows.reshape(shape_four)
    value_four = value_rows.reshape(shape_four)
    paired = jnp.stack([key_rows, value_rows])
    padded = extended(paired, (("seq", 1),), BLK)
    padded = padded.reshape(2, blk_dev + 2, BLK, heads_dev, HEAD_DIM)
    window = jnp.stack([padded[:, offset : offset + blk_dev] for offset in range(3)], axis=2)
    near_ids = (
        first_block
        + jnp.arange(blk_dev, dtype=jnp.int32)[:, None]
        + jnp.arange(-1, 2, dtype=jnp.int32)[None, :]
    )
    inside = (near_ids >= 0) & (near_ids < total_blocks)
    stacked = jnp.stack([query_rows, key_rows, value_rows]).reshape(
        3, blk_dev, BLK, heads_dev * HEAD_DIM
    )
    owned_mask = global_blocks // blk_dev == seq_index
    local_ids = jnp.where(owned_mask, global_blocks - first_block, 0)
    picked = (
        jnp.take(stacked, local_ids, axis=1).astype(jnp.float32)
        * owned_mask.astype(jnp.float32)[None, :, None, None]
    )
    glob_rows = lax.psum(picked, "seq").astype(jnp.bfloat16)
    glob_rows = glob_rows.reshape(3, glob_count, BLK, heads_dev, HEAD_DIM)
    requests, slot_ids, sources = make_requests(random_blocks, seq_count, capacity)
    incoming = lax.all_to_all(requests, "seq", split_axis=0, concat_axis=0, tiled=True)

    def by_block(row_data):
        return (
            row_data.reshape(shape_four)
            .transpose(0, 2, 1, 3)
            .reshape(blk_dev * heads_dev, BLK, HEAD_DIM)
        )

    pair_blocks = jnp.stack([by_block(key_rows), by_block(value_rows)], axis=1)
    served = pair_blocks[incoming]
    key_win, value_win = (window[0], window[1])
    win_scores = (
        jnp.einsum("jqhd,jwkhd->jhqwk", query_four, key_win, preferred_element_type=jnp.float32)
        * score_scale
    )
    win_scores = jnp.where(inside[:, None, None, :, None], win_scores, MASKED)
    glob_scores = (
        jnp.einsum("jqhd,gkhd->jhqgk", query_four, glob_rows[1], preferred_element_type=jnp.float32)
        * score_scale
    )
    split_at = 3 + glob_count
    arrived_pairs = lax.all_to_all(served, "seq", split_axis=0, concat_axis=0, tiled=True)
    tail = arrived_pairs.shape[2:]
    rand_pairs = arrived_pairs.reshape((seq_count * capacity,) + tail)[slot_ids].reshape(
        (blk_dev, heads_dev, rand_count) + tail
    )
    rand_scores = (
        jnp.einsum(
            "jqhd,jhrkd->jhqrk",
            query_four,
            rand_pairs[:, :, :, 0],
            preferred_element_type=jnp.float32,
        )
        * score_scale
    )
    peaks, totals, weights = soft_parts(
        jnp.concatenate([win_scores, glob_scores, rand_scores], axis=3)
    )
    sums_all = jnp.einsum(
        "jhqwk,jwkhd->jhqd", weights[:, :, :, 0:3], value_win, preferred_element_type=jnp.float32
    )
    sums_all = sums_all + jnp.einsum(
        "jhqgk,gkhd->jhqd",
        weights[:, :, :, 3:split_at],
        glob_rows[2],
        preferred_element_type=jnp.float32,
    )
    sums_all = sums_all + jnp.einsum(
        "jhqrk,jhrkd->jhqd",
        weights[:, :, :, split_at:],
        rand_pairs[:, :, :, 1],
        preferred_element_type=jnp.float32,
    )
    running = (peaks, totals, sums_all)
    sparse_out = (running[2] / running[1][..., None]).transpose(0, 2, 1, 3)
    full_scores = (
        jnp.einsum("gqhd,jkhd->hgqjk", glob_rows[0], key_four, preferred_element_type=jnp.float32)
        * score_scale
    )
    full_peaks, full_totals, full_weights = soft_parts(full_scores)
    full_sum = jnp.einsum(
        "hgqjk,jkhd->hgqd", full_weights, value_four, preferred_element_type=jnp.float32
    )
    merged = combined_all((full_peaks, full_totals, full_sum), "seq", merge_parts)
    glob_out = (merged[2] / merged[1][..., None]).transpose(1, 2, 0, 3)
    block_ids = first_block + jnp.arange(blk_dev, dtype=jnp.int32)
    result = sparse_out
    for glob_id in range(glob_count):
        matches = (block_ids == global_blocks[glob_id])[:, None, None, None]
        result = jnp.where(matches, glob_out[glob_id][None], result)
    return result.reshape(tokens, heads_dev * HEAD_DIM)


POOL_LIMIT = 16 * 2**20


def headed_kernel(
    seq_count, head_count, rand_count, glob_count,
    q_hbm, k_hbm, v_hbm, rand_hbm, glob_ref, out_hbm,
    k_pool, v_pool, q_pool, rand_vmem, rand_smem, p_buf, tot_buf, full_p, full_tot, full_out,
    o_buf, local_sem, send_sem, k_sem, v_sem, q_sem, o_sem, rand_sem,
):
    seq = lax.axis_index("seq")
    head = lax.axis_index("head")
    depth = seq_count // 2
    lanes = head_count // 2
    z, y = seq // 2, seq % 2
    x, core = head // 2, head % 2
    heads_dev = seq_count // 2
    span = seq_count * lanes
    blocks = 2 * span
    mine = 2 * (seq * lanes + x) + core
    group = 2 * x + seq // heads_dev
    column = seq % heads_dev
    partner = {"seq": seq, "head": 2 * x + 1 - core}
    scale = 1.0 / math.sqrt(HEAD_DIM)

    def seq_at(dz, dy):
        return (z + dz) % depth * 2 + (y + dy) % 2

    offsets = [
        (dz, dy, dx)
        for dz in list(range(1, depth)) + [0]
        for dy in range(2)
        for dx in range(lanes)
        if (dz, dy, dx) != (0, 0, 0)
    ]

    pending = []

    def remote(source, dest, sender, receiver, device):
        return pltpu.make_async_remote_copy(
            src_ref=source, dst_ref=dest, send_sem=sender, recv_sem=receiver,
            device_id=device, device_id_type=pl.DeviceIdType.MESH,
        )

    def post(source, dest, receiver, device):
        copy = remote(source, dest, send_sem.at[len(pending)], receiver, device)
        pending.append((copy, None))
        copy.start()

    def post_or_keep(source, dest, receiver, device, here):
        sender = send_sem.at[len(pending)]
        copy = remote(source, dest, sender, receiver, device)
        kept = pltpu.make_async_copy(source, dest, receiver)
        pl.when(here)(lambda: kept.start())
        pl.when(jnp.logical_not(here))(lambda: copy.start())
        pending.append((copy, jnp.logical_not(here)))

    def arrive(piece, receiver):
        remote(piece, piece, send_sem.at[0], receiver, partner).wait_recv()

    barrier = pltpu.get_barrier_semaphore()
    greeted = 0
    for ds in range(seq_count):
        for dh in range(head_count):
            if ds or dh:
                friend = {"seq": (seq + ds) % seq_count, "head": (head + dh) % head_count}
                pl.semaphore_signal(
                    barrier, inc=1, device_id=friend, device_id_type=pl.DeviceIdType.MESH
                )
                greeted += 1

    own_cols = pl.ds(pl.multiple_of((x * seq_count + seq) * HEAD_DIM, HEAD_DIM), HEAD_DIM)
    slot = mine // 2
    own = [
        pltpu.make_async_copy(k_hbm.at[:, own_cols], k_pool.at[mine + 1], local_sem.at[0]),
        pltpu.make_async_copy(q_hbm.at[:, own_cols], q_pool.at[slot], local_sem.at[1]),
        pltpu.make_async_copy(v_hbm.at[:, own_cols], v_pool.at[mine + 1], local_sem.at[2]),
    ]
    for copy in own:
        copy.start()
    blank = jnp.zeros((BLK, HEAD_DIM), jnp.bfloat16)
    for pool in (k_pool, v_pool):
        pool[0] = blank
        pool[blocks + 1] = blank
    pl.semaphore_wait(barrier, greeted)

    def scatter(source, dest, receiver):
        for dz, dy, dx in offsets:
            there, lane = seq_at(dz, dy), (x + dx) % lanes
            cols = pl.ds(pl.multiple_of((lane * seq_count + there) * HEAD_DIM, HEAD_DIM), HEAD_DIM)
            post(source.at[:, cols], dest, receiver, {"seq": there, "head": 2 * lane + core})

    for there in range(heads_dev):
        owner = head % 2 * heads_dev + there
        for other in range(2):
            post_or_keep(
                rand_hbm, rand_vmem.at[seq], rand_sem.at[seq], {"seq": owner, "head": 2 * x + other},
                (owner == seq) & (core == other),
            )
    scatter(k_hbm, k_pool.at[mine + 1], k_sem.at[mine])
    scatter(q_hbm, q_pool.at[slot], q_sem.at[slot])
    scatter(v_hbm, v_pool.at[mine + 1], v_sem.at[mine])

    def source_slot(dz, dy, dx):
        return seq_at(-dz, -dy) * lanes + (x - dx) % lanes

    def pass_on(pool, own_copy, sems):
        own_copy.wait()
        post(pool.at[mine + 1], pool.at[mine + 1], sems.at[mine], partner)
        for offset in offsets:
            block = 2 * source_slot(*offset) + core
            arrive(pool.at[block + 1], sems.at[block])
            post(pool.at[block + 1], pool.at[block + 1], sems.at[block], partner)

    def collect(pool, sems):
        for n in range(span):
            block = 2 * n + 1 - core
            arrive(pool.at[block + 1], sems.at[block])

    pass_on(k_pool, own[0], k_sem)
    for s in range(seq_count):
        arrive(rand_vmem.at[s], rand_sem.at[s])
    names = pltpu.make_async_copy(rand_vmem, rand_smem, local_sem.at[3])
    names.start()
    own[1].wait()
    for offset in offsets:
        n = source_slot(*offset)
        arrive(q_pool.at[n], q_sem.at[n])
    collect(k_pool, k_sem)
    names.wait()

    def key_set(pool, n):
        s, lane = n // lanes, n % lanes
        block = 2 * n + core
        parts = [pool[pl.ds(block, 3)].reshape(3 * BLK, HEAD_DIM)]
        parts += [pool[glob_ref[g] + 1] for g in range(glob_count)]
        parts += [
            pool[rand_smem[s, r, 2 * lane + core, column] + 1] for r in range(rand_count)
        ]
        return jnp.concatenate(parts, axis=0)

    def soften(scores):
        peaks = jnp.max(scores, axis=1, keepdims=True)
        powers = jnp.exp(scores - peaks)
        return powers.astype(jnp.bfloat16), jnp.sum(powers, axis=1, keepdims=True)

    def scored(query, keys):
        return lax.dot_general(
            query, keys, (((1,), (1,)), ((), ())), preferred_element_type=jnp.float32
        ) * scale

    for n in range(span):
        scores = scored(q_pool[n], key_set(k_pool, n))
        place = lax.broadcasted_iota(jnp.int32, scores.shape, 1) // BLK
        if n == 0:
            scores = jnp.where((place == 0) & (core == 0), MASKED, scores)
        if n == span - 1:
            scores = jnp.where((place == 2) & (core == 1), MASKED, scores)
        powers, totals = soften(scores)
        p_buf[n] = powers
        tot_buf[n] = jnp.broadcast_to(totals, (BLK, HEAD_DIM))
    every = pl.ds(1, blocks)
    for g in range(glob_count):
        powers, totals = soften(
            scored(q_pool[glob_ref[g] // 2], k_pool[every].reshape(blocks * BLK, HEAD_DIM))
        )
        full_p[g] = powers
        full_tot[g] = jnp.broadcast_to(totals, (BLK, HEAD_DIM))

    pass_on(v_pool, own[2], v_sem)
    collect(v_pool, v_sem)

    def summed(powers, values):
        return lax.dot_general(
            powers, values, (((1,), (0,)), ((), ())), preferred_element_type=jnp.float32
        )

    for g in range(glob_count):
        full_out[g] = (
            summed(full_p[g], v_pool[every].reshape(blocks * BLK, HEAD_DIM)) / full_tot[g]
        )

    def send(n):
        s, lane = n // lanes, n % lanes
        dest = out_hbm.at[
            pl.ds(pl.multiple_of((2 * lane + core) * BLK, BLK), BLK),
            pl.ds(pl.multiple_of(column * HEAD_DIM, HEAD_DIM), HEAD_DIM),
        ]
        post_or_keep(
            o_buf.at[n], dest, o_sem.at[column, 2 * lane + core], {"seq": s, "head": group},
            (seq == s) & (head == group),
        )

    for n in range(span):
        result = summed(p_buf[n], key_set(v_pool, n)) / tot_buf[n]
        for g in range(glob_count):
            result = jnp.where(glob_ref[g] == 2 * n + core, full_out[g], result)
        o_buf[n] = result.astype(jnp.bfloat16)
        if n > 0:
            send(n - 1)
    send(span - 1)
    for col in range(heads_dev):
        for row in range(head_count):
            piece = out_hbm.at[
                row * BLK : (row + 1) * BLK, col * HEAD_DIM : (col + 1) * HEAD_DIM
            ]
            arrive(piece, o_sem.at[col, row])
    for copy, when in pending:
        if when is None:
            copy.wait_send()
        else:
            pl.when(when)(lambda copy=copy: copy.wait_send())


def headed(queries, keys, values, random_blocks, global_blocks):
    seq_count, head_count = lax.axis_size("seq"), lax.axis_size("head")
    heads_dev = queries.shape[1] // HEAD_DIM // head_count
    rand_count, glob_count = random_blocks.shape[2], global_blocks.shape[0]
    names = random_blocks.transpose(2, 0, 1)
    span = seq_count * head_count // 2
    blocks = 2 * span
    width = (3 + glob_count + rand_count) * BLK
    dma = pltpu.SemaphoreType.DMA
    tile = (BLK, HEAD_DIM)
    result = pl.pallas_call(
        functools.partial(headed_kernel, seq_count, head_count, rand_count, glob_count),
        out_shape=jax.ShapeDtypeStruct((head_count * BLK, heads_dev * HEAD_DIM), jnp.bfloat16),
        in_specs=[pl.BlockSpec(memory_space=pltpu.HBM)] * 4
        + [pl.BlockSpec(memory_space=pltpu.SMEM)],
        out_specs=pl.BlockSpec(memory_space=pltpu.HBM),
        scratch_shapes=[
            pltpu.VMEM((blocks + 2,) + tile, jnp.bfloat16),
            pltpu.VMEM((blocks + 2,) + tile, jnp.bfloat16),
            pltpu.VMEM((span,) + tile, jnp.bfloat16),
            pltpu.VMEM((seq_count,) + names.shape, jnp.int32),
            pltpu.SMEM((seq_count,) + names.shape, jnp.int32),
            pltpu.VMEM((span, BLK, width), jnp.bfloat16),
            pltpu.VMEM((span,) + tile, jnp.float32),
            pltpu.VMEM((glob_count, BLK, blocks * BLK), jnp.bfloat16),
            pltpu.VMEM((glob_count,) + tile, jnp.float32),
            pltpu.VMEM((glob_count,) + tile, jnp.float32),
            pltpu.VMEM((span,) + tile, jnp.bfloat16),
            dma((4,)),
            dma((6 * span + 2 * heads_dev,)),
            dma((blocks,)),
            dma((blocks,)),
            dma((span,)),
            dma((heads_dev, head_count)),
            dma((seq_count,)),
        ],
        compiler_params=pltpu.CompilerParams(
            collective_id=0, has_side_effects=True
        ),
    )(queries, keys, values, names, global_blocks)
    return result.astype(jnp.float32)


def shards(queries, keys, values, random_blocks, global_blocks):
    seq_count, head_count = lax.axis_size("seq"), lax.axis_size("head")
    rows, width = queries.shape
    span = seq_count * head_count // 2
    fits = 6 * rows * width * span // head_count <= POOL_LIMIT
    even = seq_count % 2 == 0 and head_count % 2 == 0
    if fits and even and rows == BLK and width == span * HEAD_DIM:
        return headed(queries, keys, values, random_blocks, global_blocks)
    return exchanged(queries, keys, values, random_blocks, global_blocks)


def solution(mesh):
    in_specs = (
        P(("seq", "head"), None),
        P(("seq", "head"), None),
        P(("seq", "head"), None),
        P("seq", "head", None),
        P(),
    )
    out_specs = P("seq", "head")
    return jax.shard_map(shards, mesh=mesh, in_specs=in_specs, out_specs=out_specs, check_vma=False)
```

```python
import functools
import math

import jax
import jax.numpy as jnp
from jax import lax
from jax.experimental import pallas as pl
from jax.experimental.pallas import tpu as pltpu
from jax.sharding import PartitionSpec as P

HEAD_DIM = 128
BLK = 64


MASKED = -1e30


def extended(block, sides, width):
    for axis, dim in sides:
        count = lax.axis_size(axis)
        forward = [(i, i + 1) for i in range(count - 1)]
        backward = [(target, source) for source, target in forward]
        low = lax.ppermute(
            lax.slice_in_dim(block, block.shape[dim] - width, None, axis=dim), axis, forward
        )
        high = lax.ppermute(lax.slice_in_dim(block, 0, width, axis=dim), axis, backward)
        block = jnp.concatenate([low, block, high], axis=dim)
    return block


def combined_all(value, axis, join):
    pieces = jax.tree.map(lambda part: lax.all_gather(part, axis), value)
    head = jax.tree.map(lambda part: part[0], pieces)
    tail = jax.tree.map(lambda part: part[1:], pieces)
    so_far, _ = lax.scan(lambda so_far, slab: (join(so_far, slab), None), head, tail)
    return so_far


def merge_parts(former, latter):
    peaks = jnp.maximum(former[0], latter[0])
    former_fade = jnp.exp(former[0] - peaks)
    latter_fade = jnp.exp(latter[0] - peaks)
    return (
        peaks,
        former[1] * former_fade + latter[1] * latter_fade,
        former[2] * former_fade[..., None] + latter[2] * latter_fade[..., None],
    )


def soft_parts(scores):
    peaks = jnp.max(scores, axis=(-2, -1))
    powers = jnp.exp(scores - peaks[..., None, None])
    return (peaks, jnp.sum(powers, axis=(-2, -1)), powers.astype(jnp.bfloat16))


def make_requests(rand_lists, seq_count, capacity):
    blk_dev, heads_dev, rand_count = rand_lists.shape
    flat_list = rand_lists.reshape(-1)
    owners = flat_list // blk_dev
    head_ids = jnp.broadcast_to(
        jnp.arange(heads_dev, dtype=jnp.int32)[None, :, None], rand_lists.shape
    ).reshape(-1)
    item_ids = flat_list % blk_dev * heads_dev + head_ids
    position = jnp.arange(flat_list.shape[0], dtype=jnp.int32)
    earlier = (owners[:, None] == owners[None, :]) & (position[None, :] < position[:, None])
    slot_ids = owners * capacity + jnp.sum(earlier.astype(jnp.int32), axis=1)
    requests = jnp.zeros((seq_count * capacity,), jnp.int32).at[slot_ids].set(item_ids)
    sources = jnp.zeros((seq_count * capacity,), jnp.int32).at[slot_ids].set(position)
    return (requests.reshape(seq_count, capacity), slot_ids, sources)


def exchanged(queries, keys, values, random_blocks, global_blocks):
    seq_count = lax.axis_size("seq")
    seq_index = lax.axis_index("seq")
    query_rows, key_rows, value_rows = (
        lax.all_to_all(queries, "head", split_axis=1, concat_axis=0, tiled=True),
        lax.all_to_all(keys, "head", split_axis=1, concat_axis=0, tiled=True),
        lax.all_to_all(values, "head", split_axis=1, concat_axis=0, tiled=True),
    )
    tokens = query_rows.shape[0]
    blk_dev = tokens // BLK
    heads_dev = query_rows.shape[1] // HEAD_DIM
    rand_count = random_blocks.shape[2]
    glob_count = global_blocks.shape[0]
    total_blocks = blk_dev * seq_count
    first_block = seq_index * blk_dev
    capacity = (blk_dev * heads_dev * rand_count * 3 // 2 + seq_count - 1) // seq_count
    score_scale = 1.0 / math.sqrt(HEAD_DIM)
    shape_four = (blk_dev, BLK, heads_dev, HEAD_DIM)
    query_four = query_rows.reshape(shape_four)
    key_four = key_rows.reshape(shape_four)
    value_four = value_rows.reshape(shape_four)
    paired = jnp.stack([key_rows, value_rows])
    padded = extended(paired, (("seq", 1),), BLK)
    padded = padded.reshape(2, blk_dev + 2, BLK, heads_dev, HEAD_DIM)
    window = jnp.stack([padded[:, offset : offset + blk_dev] for offset in range(3)], axis=2)
    near_ids = (
        first_block
        + jnp.arange(blk_dev, dtype=jnp.int32)[:, None]
        + jnp.arange(-1, 2, dtype=jnp.int32)[None, :]
    )
    inside = (near_ids >= 0) & (near_ids < total_blocks)
    stacked = jnp.stack([query_rows, key_rows, value_rows]).reshape(
        3, blk_dev, BLK, heads_dev * HEAD_DIM
    )
    owned_mask = global_blocks // blk_dev == seq_index
    local_ids = jnp.where(owned_mask, global_blocks - first_block, 0)
    picked = (
        jnp.take(stacked, local_ids, axis=1).astype(jnp.float32)
        * owned_mask.astype(jnp.float32)[None, :, None, None]
    )
    glob_rows = lax.psum(picked, "seq").astype(jnp.bfloat16)
    glob_rows = glob_rows.reshape(3, glob_count, BLK, heads_dev, HEAD_DIM)
    requests, slot_ids, sources = make_requests(random_blocks, seq_count, capacity)
    incoming = lax.all_to_all(requests, "seq", split_axis=0, concat_axis=0, tiled=True)

    def by_block(row_data):
        return (
            row_data.reshape(shape_four)
            .transpose(0, 2, 1, 3)
            .reshape(blk_dev * heads_dev, BLK, HEAD_DIM)
        )

    pair_blocks = jnp.stack([by_block(key_rows), by_block(value_rows)], axis=1)
    served = pair_blocks[incoming]
    key_win, value_win = (window[0], window[1])
    win_scores = (
        jnp.einsum("jqhd,jwkhd->jhqwk", query_four, key_win, preferred_element_type=jnp.float32)
        * score_scale
    )
    win_scores = jnp.where(inside[:, None, None, :, None], win_scores, MASKED)
    glob_scores = (
        jnp.einsum("jqhd,gkhd->jhqgk", query_four, glob_rows[1], preferred_element_type=jnp.float32)
        * score_scale
    )
    split_at = 3 + glob_count
    arrived_pairs = lax.all_to_all(served, "seq", split_axis=0, concat_axis=0, tiled=True)
    tail = arrived_pairs.shape[2:]
    rand_pairs = arrived_pairs.reshape((seq_count * capacity,) + tail)[slot_ids].reshape(
        (blk_dev, heads_dev, rand_count) + tail
    )
    rand_scores = (
        jnp.einsum(
            "jqhd,jhrkd->jhqrk",
            query_four,
            rand_pairs[:, :, :, 0],
            preferred_element_type=jnp.float32,
        )
        * score_scale
    )
    peaks, totals, weights = soft_parts(
        jnp.concatenate([win_scores, glob_scores, rand_scores], axis=3)
    )
    sums_all = jnp.einsum(
        "jhqwk,jwkhd->jhqd", weights[:, :, :, 0:3], value_win, preferred_element_type=jnp.float32
    )
    sums_all = sums_all + jnp.einsum(
        "jhqgk,gkhd->jhqd",
        weights[:, :, :, 3:split_at],
        glob_rows[2],
        preferred_element_type=jnp.float32,
    )
    sums_all = sums_all + jnp.einsum(
        "jhqrk,jhrkd->jhqd",
        weights[:, :, :, split_at:],
        rand_pairs[:, :, :, 1],
        preferred_element_type=jnp.float32,
    )
    running = (peaks, totals, sums_all)
    sparse_out = (running[2] / running[1][..., None]).transpose(0, 2, 1, 3)
    full_scores = (
        jnp.einsum("gqhd,jkhd->hgqjk", glob_rows[0], key_four, preferred_element_type=jnp.float32)
        * score_scale
    )
    full_peaks, full_totals, full_weights = soft_parts(full_scores)
    full_sum = jnp.einsum(
        "hgqjk,jkhd->hgqd", full_weights, value_four, preferred_element_type=jnp.float32
    )
    merged = combined_all((full_peaks, full_totals, full_sum), "seq", merge_parts)
    glob_out = (merged[2] / merged[1][..., None]).transpose(1, 2, 0, 3)
    block_ids = first_block + jnp.arange(blk_dev, dtype=jnp.int32)
    result = sparse_out
    for glob_id in range(glob_count):
        matches = (block_ids == global_blocks[glob_id])[:, None, None, None]
        result = jnp.where(matches, glob_out[glob_id][None], result)
    return result.reshape(tokens, heads_dev * HEAD_DIM)


POOL_LIMIT = 16 * 2**20


def headed_kernel(
    seq_count, head_count, rand_count,
    q_hbm, k_hbm, v_hbm, rand_hbm, glob_ref, out_ref,
    k_pool, v_pool, q_early, q_late, rand_own, rand_tile, rand_vmem, rand_smem, p_buf, tot_buf, full_p, full_tot,
    full_out, o_buf, local_sem, send_sem, pass_sem, rand_send, o_send,
    k_sem, v_sem, q_sem, o_sem, rand_sem,
):
    seq = lax.axis_index("seq")
    head = lax.axis_index("head")
    depth = seq_count // 2
    lanes = head_count // 2
    z, y = seq // 2, seq % 2
    x, core = head // 2, head % 2
    heads_dev = seq_count // 2
    span = seq_count * lanes
    blocks = 2 * span
    late_lanes = lanes // 2
    early_lanes = lanes - late_lanes
    slot = seq * lanes + x
    mine = 2 * slot + core
    group = 2 * x + seq // heads_dev
    column = seq % heads_dev
    partner = {"seq": seq, "head": 2 * x + 1 - core}
    last = blocks - 1
    other = jnp.clip(glob_ref[0] + glob_ref[1] - last, 0, last)
    scale = 1.0 / math.sqrt(HEAD_DIM)

    def device(there, lane):
        return {"seq": there, "head": 2 * lane + core}

    def remote(source, dest, sender, receiver, target):
        return pltpu.make_async_remote_copy(
            src_ref=source, dst_ref=dest, send_sem=sender, recv_sem=receiver,
            device_id=target, device_id_type=pl.DeviceIdType.MESH,
        )

    def arrive(piece, receiver):
        remote(piece, piece, local_sem.at[0], receiver, partner).wait_recv()

    def leave(piece, sender):
        remote(piece, piece, sender, local_sem.at[0], partner).wait_send()

    barrier = pltpu.get_barrier_semaphore()
    friends = 0
    for ds in range(seq_count):
        for dh in range(head_count):
            if ds or dh:
                friend = {"seq": (seq + ds) % seq_count, "head": (head + dh) % head_count}
                pl.semaphore_signal(
                    barrier, inc=1, device_id=friend, device_id_type=pl.DeviceIdType.MESH
                )
                friends += 1

    def columns(there, lane):
        return pl.ds(pl.multiple_of((lane * seq_count + there) * HEAD_DIM, HEAD_DIM), HEAD_DIM)

    here = columns(seq, x)
    pltpu.make_async_copy(k_hbm.at[:, here], k_pool.at[mine + 1], k_sem.at[mine]).start()
    pltpu.make_async_copy(v_hbm.at[:, here], v_pool.at[mine + 1], v_sem.at[mine]).start()

    pltpu.make_async_copy(
        q_hbm.at[:, here], q_early.at[seq * early_lanes], q_sem.at[slot]
    ).start()
    blank = jnp.zeros((BLK, HEAD_DIM), jnp.bfloat16)
    for pool in (k_pool, v_pool):
        pool[0] = blank
        pool[blocks + 1] = blank

    own_names = pltpu.make_async_copy(
        rand_hbm, rand_own.at[pl.ds(0, rand_count)], local_sem.at[1]
    )
    own_names.start()
    rand_tile[...] = jnp.zeros_like(rand_tile)
    own_names.wait()
    for r in range(rand_count):
        rand_tile[:head_count, r * heads_dev : (r + 1) * heads_dev] = rand_own[r]
    pl.semaphore_wait(barrier, friends)

    steps = list(range(1, depth)) + [0]

    def push(kind, source, dest, receiver, lane_steps):
        for step in steps:
            for dy in range(2):
                for dx in lane_steps:
                    if step or dy or dx:
                        there, lane = 2 * ((z + step) % depth) + (y + dy) % 2, (x + dx) % lanes
                        sender = send_sem.at[kind, (step * 2 + dy) * lanes + dx]
                        remote(
                            source.at[:, columns(there, lane)], dest(dx), sender, receiver,
                            device(there, lane),
                        ).start()

    def post_or_keep(source, dest, sender, receiver, target, at_home):
        copy = remote(source, dest, sender, receiver, target)
        kept = pltpu.make_async_copy(source, dest, receiver)
        pl.when(at_home)(lambda: kept.start())
        pl.when(jnp.logical_not(at_home))(lambda: copy.start())

    lead = seq // heads_dev

    def owner_of(there):
        return head % 2 * heads_dev + there

    everyone = range(lanes)
    push(0, k_hbm, lambda dx: k_pool.at[mine + 1], k_sem.at[mine], everyone)
    for there in range(heads_dev):
        post_or_keep(
            rand_tile, rand_vmem.at[seq], rand_send.at[there], rand_sem.at[seq],
            {"seq": owner_of(there), "head": head}, owner_of(there) == seq,
        )
    push(
        2, q_hbm, lambda dx: q_early.at[seq * early_lanes + dx], q_sem.at[slot], range(early_lanes)
    )
    push(1, v_hbm, lambda dx: v_pool.at[mine + 1], v_sem.at[mine], everyone)
    push(
        2, q_hbm, lambda dx: q_late.at[seq * late_lanes + dx - early_lanes], q_sem.at[slot],
        range(early_lanes, lanes),
    )

    def slots(lane_steps):
        return [(s, dx, (x - dx) % lanes) for s in range(seq_count) for dx in lane_steps]

    early = slots(range(early_lanes))
    late = slots(range(early_lanes, lanes))

    def pass_on(kind, pool, sems):
        arrivals = [
            (2 * ((z - step) % depth) + (y + dy) % 2, (x - dx) % lanes)
            for step in steps[::-1]
            for dy in range(2)
            for dx in everyone
        ]
        for place, (s, lane) in enumerate(arrivals):
            block = 2 * (s * lanes + lane) + core
            piece = pool.at[block + 1]
            arrive(piece, sems.at[block])
            remote(piece, piece, pass_sem.at[kind, place], sems.at[block], partner).start()

    def collect(pool, sems):
        for n in range(span):
            block = 2 * n + 1 - core
            arrive(pool.at[block + 1], sems.at[block])

    pass_on(0, k_pool, k_sem)
    shared = remote(rand_vmem, rand_vmem, rand_send.at[heads_dev], rand_sem.at[seq_count], partner)

    def share_names():
        for s in range(seq_count):
            arrive(rand_vmem.at[s], rand_sem.at[s])
        shared.start()

    pl.when(core == lead)(share_names)
    pl.when(core != lead)(lambda: shared.wait_recv())
    names = pltpu.make_async_copy(rand_vmem, rand_smem, local_sem.at[1])
    names.start()
    for s, dx, lane in early:
        arrive(q_early.at[s * early_lanes + dx], q_sem.at[s * lanes + lane])
    collect(k_pool, k_sem)
    names.wait()

    def key_set(pool, s, lane):
        parts = [pool[pl.ds(2 * (s * lanes + lane) + core, 3)].reshape(3 * BLK, HEAD_DIM)]
        parts += [pool[glob_ref[g] + 1] for g in range(2)]
        parts += [
            pool[rand_smem[s, 2 * lane + core, r * heads_dev + column] + 1] for r in range(rand_count)
        ]
        return jnp.concatenate(parts, axis=0)

    def soften(scores):
        peaks = jnp.max(scores, axis=1, keepdims=True)
        powers = jnp.exp(scores - peaks)
        totals = jnp.sum(powers, axis=1, keepdims=True)
        return powers.astype(jnp.bfloat16), jnp.broadcast_to(totals, (totals.shape[0], HEAD_DIM))

    def scored(query, keys):
        return lax.dot_general(
            query, keys, (((1,), (1,)), ((), ())), preferred_element_type=jnp.float32
        ) * scale

    def summed(powers, values):
        return lax.dot_general(
            powers, values, (((1,), (0,)), ((), ())), preferred_element_type=jnp.float32
        )

    edge = 4 * BLK

    def sparse_scores(query, s, lane):
        scores = scored(query, key_set(k_pool, s, lane))
        near = scores[:, :edge]
        place = lax.broadcasted_iota(jnp.int32, near.shape, 1) // BLK
        block = 2 * (s * lanes + lane) + core
        outside = ((place == 0) & (block == 0)) | ((place == 2) & (block == last))
        return jnp.concatenate([jnp.where(outside, MASKED, near), scores[:, edge:]], axis=1)

    every = pl.ds(1, blocks)

    def whole(pool):
        return pool[every].reshape(blocks * BLK, HEAD_DIM)

    for n, (s, dx, lane) in enumerate(early):
        p_buf[n], tot_buf[n] = soften(
            sparse_scores(q_early[s * early_lanes + dx], s, lane)
        )
    other_seq = other // head_count
    other_step = (x - other % head_count // 2) % lanes
    last_step = (x - lanes + 1) % lanes

    def pair(pool, count, first):
        last_place = (seq_count - 1) * count + jnp.clip(last_step - first, 0, count - 1)
        other_place = other_seq * count + jnp.clip(other_step - first, 0, count - 1)
        return jnp.concatenate([pool[last_place], pool[other_place]], axis=0)

    full_p[...], full_tot[...] = soften(scored(pair(q_early, early_lanes, 0), whole(k_pool)))

    pass_on(1, v_pool, v_sem)
    collect(v_pool, v_sem)
    full_out[...] = summed(full_p[...], whole(v_pool)) / full_tot[...]

    def send(s, lane):
        n = s * lanes + lane
        rows = pl.ds(pl.multiple_of((2 * lane + core) * BLK, BLK), BLK)
        cols = pl.ds(pl.multiple_of(column * HEAD_DIM, HEAD_DIM), HEAD_DIM)
        post_or_keep(
            o_buf.at[n], out_ref.at[rows, cols], o_send.at[n], o_sem.at[column, 2 * lane + core],
            {"seq": s, "head": group}, (seq == s) & (head == group),
        )

    def finish(result, s, lane):
        block = 2 * (s * lanes + lane) + core
        result = jnp.where(last == block, full_out[:BLK], result)
        result = jnp.where(other == block, full_out[BLK:], result)
        o_buf[s * lanes + lane] = result.astype(jnp.bfloat16)

    ready = None
    for n, (s, dx, lane) in enumerate(early):
        finish(summed(p_buf[n], key_set(v_pool, s, lane)) / tot_buf[n], s, lane)
        if ready:
            send(*ready)
        ready = (s, lane)
    send(*ready)
    if late:
        for s, dx, lane in late:
            arrive(q_late.at[s * late_lanes + dx - early_lanes], q_sem.at[s * lanes + lane])
        powers, totals = soften(scored(pair(q_late, late_lanes, early_lanes), whole(k_pool)))
        full_out[...] = summed(powers, whole(v_pool)) / totals
        ready = None
        for s, dx, lane in late:
            query = q_late[s * late_lanes + dx - early_lanes]
            powers, totals = soften(sparse_scores(query, s, lane))
            finish(summed(powers, key_set(v_pool, s, lane)) / totals, s, lane)
            if ready:
                send(*ready)
            ready = (s, lane)
        send(*ready)

    tile = k_pool.at[0]
    for kind in range(3):
        for n in range(1, span):
            leave(tile, send_sem.at[kind, n])
    for kind in range(2):
        for place in range(span):
            leave(tile, pass_sem.at[kind, place])
    for there in range(heads_dev):
        pl.when(owner_of(there) != seq)(
            lambda there=there: leave(rand_tile, rand_send.at[there])
        )
    pl.when(core == lead)(lambda: shared.wait_send())
    for s, dx, lane in early + late:
        pl.when((seq != s) | (head != group))(
            lambda s=s, lane=lane: leave(tile, o_send.at[s * lanes + lane])
        )
    for col in range(heads_dev):
        for row in range(head_count):
            piece = out_ref.at[
                row * BLK : (row + 1) * BLK, col * HEAD_DIM : (col + 1) * HEAD_DIM
            ]
            arrive(piece, o_sem.at[col, row])


def headed(queries, keys, values, random_blocks, global_blocks):
    seq_count, head_count = lax.axis_size("seq"), lax.axis_size("head")
    heads_dev = queries.shape[1] // HEAD_DIM // head_count
    rand_count = random_blocks.shape[2]
    names = random_blocks.transpose(2, 0, 1)
    lanes = head_count // 2
    late_lanes = lanes // 2
    early_count, late_count = seq_count * (lanes - late_lanes), max(seq_count * late_lanes, 1)
    span = seq_count * lanes
    blocks = 2 * span
    width = (5 + rand_count) * BLK
    dma = pltpu.SemaphoreType.DMA
    tile, name_tile = (BLK, HEAD_DIM), (8, 128)

    def bf16(*shape):
        return pltpu.VMEM(shape, jnp.bfloat16)

    def f32(*shape):
        return pltpu.VMEM(shape, jnp.float32)

    result = pl.pallas_call(
        functools.partial(headed_kernel, seq_count, head_count, rand_count),
        out_shape=bf16(head_count * BLK, heads_dev * HEAD_DIM),
        in_specs=[pl.BlockSpec(memory_space=pltpu.HBM)] * 4
        + [pl.BlockSpec(memory_space=pltpu.SMEM)],
        out_specs=pl.BlockSpec(memory_space=pl.ANY),
        scratch_shapes=[
            bf16(blocks + 2, *tile),
            bf16(blocks + 2, *tile),
            bf16(early_count, *tile),
            bf16(late_count, *tile),
            pltpu.VMEM((rand_count + 1,) + names.shape[1:], jnp.int32),
            pltpu.VMEM(name_tile, jnp.int32),
            pltpu.VMEM((seq_count,) + name_tile, jnp.int32),
            pltpu.SMEM((seq_count,) + name_tile, jnp.int32),
            bf16(early_count, BLK, width),
            f32(early_count, *tile),
            bf16(2 * BLK, blocks * BLK),
            f32(2 * BLK, HEAD_DIM),
            f32(2 * BLK, HEAD_DIM),
            bf16(span, *tile),
            dma((2,)),
            dma((3, span)),
            dma((2, span)),
            dma((heads_dev + 1,)),
            dma((span,)),
            dma((blocks,)),
            dma((blocks,)),
            dma((span,)),
            dma((heads_dev, head_count)),
            dma((seq_count + 1,)),
        ],
        compiler_params=pltpu.CompilerParams(
            collective_id=0, has_side_effects=True
        ),
    )(queries, keys, values, names, global_blocks)
    return result.astype(jnp.float32)


def shards(queries, keys, values, random_blocks, global_blocks):
    seq_count, head_count = lax.axis_size("seq"), lax.axis_size("head")
    rows, width = queries.shape
    span = seq_count * head_count // 2
    fits = 6 * rows * width * span // head_count <= POOL_LIMIT
    even = seq_count % 2 == 0 and head_count % 2 == 0 and global_blocks.shape[0] == 2
    if fits and even and rows == BLK and width == span * HEAD_DIM:
        return headed(queries, keys, values, random_blocks, global_blocks)
    return exchanged(queries, keys, values, random_blocks, global_blocks)


def solution(mesh):
    in_specs = (
        P(("seq", "head"), None),
        P(("seq", "head"), None),
        P(("seq", "head"), None),
        P("seq", "head", None),
        P(),
    )
    out_specs = P("seq", "head")
    return jax.shard_map(shards, mesh=mesh, in_specs=in_specs, out_specs=out_specs, check_vma=False)
```

```python
import functools
import math

import jax
import jax.numpy as jnp
from jax import lax
from jax.experimental import pallas as pl
from jax.experimental.pallas import tpu as pltpu
from jax.sharding import PartitionSpec as P

HEAD_DIM = 128
BLK = 64


MASKED = -1e30


def extended(block, sides, width):
    for axis, dim in sides:
        count = lax.axis_size(axis)
        forward = [(i, i + 1) for i in range(count - 1)]
        backward = [(target, source) for source, target in forward]
        low = lax.ppermute(
            lax.slice_in_dim(block, block.shape[dim] - width, None, axis=dim), axis, forward
        )
        high = lax.ppermute(lax.slice_in_dim(block, 0, width, axis=dim), axis, backward)
        block = jnp.concatenate([low, block, high], axis=dim)
    return block


def combined_all(value, axis, join):
    pieces = jax.tree.map(lambda part: lax.all_gather(part, axis), value)
    head = jax.tree.map(lambda part: part[0], pieces)
    tail = jax.tree.map(lambda part: part[1:], pieces)
    so_far, _ = lax.scan(lambda so_far, slab: (join(so_far, slab), None), head, tail)
    return so_far


def merge_parts(former, latter):
    peaks = jnp.maximum(former[0], latter[0])
    former_fade = jnp.exp(former[0] - peaks)
    latter_fade = jnp.exp(latter[0] - peaks)
    return (
        peaks,
        former[1] * former_fade + latter[1] * latter_fade,
        former[2] * former_fade[..., None] + latter[2] * latter_fade[..., None],
    )


def soft_parts(scores):
    peaks = jnp.max(scores, axis=(-2, -1))
    powers = jnp.exp(scores - peaks[..., None, None])
    return (peaks, jnp.sum(powers, axis=(-2, -1)), powers.astype(jnp.bfloat16))


def make_requests(rand_lists, seq_count, capacity):
    blk_dev, heads_dev, rand_count = rand_lists.shape
    flat_list = rand_lists.reshape(-1)
    owners = flat_list // blk_dev
    head_ids = jnp.broadcast_to(
        jnp.arange(heads_dev, dtype=jnp.int32)[None, :, None], rand_lists.shape
    ).reshape(-1)
    item_ids = flat_list % blk_dev * heads_dev + head_ids
    position = jnp.arange(flat_list.shape[0], dtype=jnp.int32)
    earlier = (owners[:, None] == owners[None, :]) & (position[None, :] < position[:, None])
    slot_ids = owners * capacity + jnp.sum(earlier.astype(jnp.int32), axis=1)
    requests = jnp.zeros((seq_count * capacity,), jnp.int32).at[slot_ids].set(item_ids)
    sources = jnp.zeros((seq_count * capacity,), jnp.int32).at[slot_ids].set(position)
    return (requests.reshape(seq_count, capacity), slot_ids, sources)


def exchanged(queries, keys, values, random_blocks, global_blocks):
    seq_count = lax.axis_size("seq")
    seq_index = lax.axis_index("seq")
    query_rows, key_rows, value_rows = (
        lax.all_to_all(queries, "head", split_axis=1, concat_axis=0, tiled=True),
        lax.all_to_all(keys, "head", split_axis=1, concat_axis=0, tiled=True),
        lax.all_to_all(values, "head", split_axis=1, concat_axis=0, tiled=True),
    )
    tokens = query_rows.shape[0]
    blk_dev = tokens // BLK
    heads_dev = query_rows.shape[1] // HEAD_DIM
    rand_count = random_blocks.shape[2]
    glob_count = global_blocks.shape[0]
    total_blocks = blk_dev * seq_count
    first_block = seq_index * blk_dev
    capacity = (blk_dev * heads_dev * rand_count * 3 // 2 + seq_count - 1) // seq_count
    score_scale = 1.0 / math.sqrt(HEAD_DIM)
    shape_four = (blk_dev, BLK, heads_dev, HEAD_DIM)
    query_four = query_rows.reshape(shape_four)
    key_four = key_rows.reshape(shape_four)
    value_four = value_rows.reshape(shape_four)
    paired = jnp.stack([key_rows, value_rows])
    padded = extended(paired, (("seq", 1),), BLK)
    padded = padded.reshape(2, blk_dev + 2, BLK, heads_dev, HEAD_DIM)
    window = jnp.stack([padded[:, offset : offset + blk_dev] for offset in range(3)], axis=2)
    near_ids = (
        first_block
        + jnp.arange(blk_dev, dtype=jnp.int32)[:, None]
        + jnp.arange(-1, 2, dtype=jnp.int32)[None, :]
    )
    inside = (near_ids >= 0) & (near_ids < total_blocks)
    stacked = jnp.stack([query_rows, key_rows, value_rows]).reshape(
        3, blk_dev, BLK, heads_dev * HEAD_DIM
    )
    owned_mask = global_blocks // blk_dev == seq_index
    local_ids = jnp.where(owned_mask, global_blocks - first_block, 0)
    picked = (
        jnp.take(stacked, local_ids, axis=1).astype(jnp.float32)
        * owned_mask.astype(jnp.float32)[None, :, None, None]
    )
    glob_rows = lax.psum(picked, "seq").astype(jnp.bfloat16)
    glob_rows = glob_rows.reshape(3, glob_count, BLK, heads_dev, HEAD_DIM)
    requests, slot_ids, sources = make_requests(random_blocks, seq_count, capacity)
    incoming = lax.all_to_all(requests, "seq", split_axis=0, concat_axis=0, tiled=True)

    def by_block(row_data):
        return (
            row_data.reshape(shape_four)
            .transpose(0, 2, 1, 3)
            .reshape(blk_dev * heads_dev, BLK, HEAD_DIM)
        )

    pair_blocks = jnp.stack([by_block(key_rows), by_block(value_rows)], axis=1)
    served = pair_blocks[incoming]
    key_win, value_win = (window[0], window[1])
    win_scores = (
        jnp.einsum("jqhd,jwkhd->jhqwk", query_four, key_win, preferred_element_type=jnp.float32)
        * score_scale
    )
    win_scores = jnp.where(inside[:, None, None, :, None], win_scores, MASKED)
    glob_scores = (
        jnp.einsum("jqhd,gkhd->jhqgk", query_four, glob_rows[1], preferred_element_type=jnp.float32)
        * score_scale
    )
    split_at = 3 + glob_count
    arrived_pairs = lax.all_to_all(served, "seq", split_axis=0, concat_axis=0, tiled=True)
    tail = arrived_pairs.shape[2:]
    rand_pairs = arrived_pairs.reshape((seq_count * capacity,) + tail)[slot_ids].reshape(
        (blk_dev, heads_dev, rand_count) + tail
    )
    rand_scores = (
        jnp.einsum(
            "jqhd,jhrkd->jhqrk",
            query_four,
            rand_pairs[:, :, :, 0],
            preferred_element_type=jnp.float32,
        )
        * score_scale
    )
    peaks, totals, weights = soft_parts(
        jnp.concatenate([win_scores, glob_scores, rand_scores], axis=3)
    )
    sums_all = jnp.einsum(
        "jhqwk,jwkhd->jhqd", weights[:, :, :, 0:3], value_win, preferred_element_type=jnp.float32
    )
    sums_all = sums_all + jnp.einsum(
        "jhqgk,gkhd->jhqd",
        weights[:, :, :, 3:split_at],
        glob_rows[2],
        preferred_element_type=jnp.float32,
    )
    sums_all = sums_all + jnp.einsum(
        "jhqrk,jhrkd->jhqd",
        weights[:, :, :, split_at:],
        rand_pairs[:, :, :, 1],
        preferred_element_type=jnp.float32,
    )
    running = (peaks, totals, sums_all)
    sparse_out = (running[2] / running[1][..., None]).transpose(0, 2, 1, 3)
    full_scores = (
        jnp.einsum("gqhd,jkhd->hgqjk", glob_rows[0], key_four, preferred_element_type=jnp.float32)
        * score_scale
    )
    full_peaks, full_totals, full_weights = soft_parts(full_scores)
    full_sum = jnp.einsum(
        "hgqjk,jkhd->hgqd", full_weights, value_four, preferred_element_type=jnp.float32
    )
    merged = combined_all((full_peaks, full_totals, full_sum), "seq", merge_parts)
    glob_out = (merged[2] / merged[1][..., None]).transpose(1, 2, 0, 3)
    block_ids = first_block + jnp.arange(blk_dev, dtype=jnp.int32)
    result = sparse_out
    for glob_id in range(glob_count):
        matches = (block_ids == global_blocks[glob_id])[:, None, None, None]
        result = jnp.where(matches, glob_out[glob_id][None], result)
    return result.reshape(tokens, heads_dev * HEAD_DIM)


POOL_LIMIT = 16 * 2**20


def headed_kernel(
    seq_count, head_count, rand_count,
    q_hbm, k_hbm, v_hbm, rand_hbm, glob_ref, out_ref,
    k_pool, v_pool, q_early, q_late, rand_own, rand_tile, rand_vmem, rand_smem, p_buf, tot_buf, full_p, full_tot,
    full_out, o_buf, local_sem, go_sem, send_sem, pass_sem, rand_send, o_send,
    k_sem, v_sem, q_sem, o_sem, rand_sem,
):
    seq = lax.axis_index("seq")
    head = lax.axis_index("head")
    depth = seq_count // 2
    lanes = head_count // 2
    z, y = seq // 2, seq % 2
    x, core = head // 2, head % 2
    heads_dev = seq_count // 2
    span = seq_count * lanes
    blocks = 2 * span
    late_lanes = lanes // 2
    early_lanes = lanes - late_lanes
    slot = seq * lanes + x
    mine = 2 * slot + core
    group = 2 * x + seq // heads_dev
    column = seq % heads_dev
    partner = {"seq": seq, "head": 2 * x + 1 - core}
    last = blocks - 1
    other = jnp.clip(glob_ref[0] + glob_ref[1] - last, 0, last)
    scale = 1.0 / math.sqrt(HEAD_DIM)

    def device(there, lane):
        return {"seq": there, "head": 2 * lane + core}

    def remote(source, dest, sender, receiver, target):
        return pltpu.make_async_remote_copy(
            src_ref=source, dst_ref=dest, send_sem=sender, recv_sem=receiver,
            device_id=target, device_id_type=pl.DeviceIdType.MESH,
        )

    def arrive(piece, receiver):
        remote(piece, piece, local_sem.at[0], receiver, partner).wait_recv()

    def leave(piece, sender):
        remote(piece, piece, sender, local_sem.at[0], partner).wait_send()

    half = depth // 2
    middle = (z == half - 1) | (z == half)
    across = jnp.where(z < half, seq + 2, seq - 2)
    barrier = pltpu.get_barrier_semaphore()

    def signal(semaphore, target):
        pl.semaphore_signal(
            semaphore, inc=1, device_id=target, device_id_type=pl.DeviceIdType.MESH
        )

    for there in range(seq_count):
        if there // 2 not in (half - 1, half):
            for twin in range(head_count):
                pl.when((seq != there) | (head != twin))(
                    lambda there=there, twin=twin: signal(barrier, {"seq": there, "head": twin})
                )
    pl.when(middle)(lambda: signal(barrier, {"seq": across, "head": head}))

    def columns(there, lane):
        return pl.ds(pl.multiple_of((lane * seq_count + there) * HEAD_DIM, HEAD_DIM), HEAD_DIM)

    here = columns(seq, x)
    pltpu.make_async_copy(k_hbm.at[:, here], k_pool.at[mine + 1], k_sem.at[mine]).start()
    pltpu.make_async_copy(v_hbm.at[:, here], v_pool.at[mine + 1], v_sem.at[mine]).start()

    pltpu.make_async_copy(
        q_hbm.at[:, here], q_early.at[seq * early_lanes], q_sem.at[slot]
    ).start()
    blank = jnp.zeros((BLK, HEAD_DIM), jnp.bfloat16)
    for pool in (k_pool, v_pool):
        pool[0] = blank
        pool[blocks + 1] = blank

    own_names = pltpu.make_async_copy(
        rand_hbm, rand_own.at[pl.ds(0, rand_count)], local_sem.at[1]
    )
    own_names.start()
    rand_tile[...] = jnp.zeros_like(rand_tile)
    own_names.wait()
    for r in range(rand_count):
        rand_tile[:head_count, r * heads_dev : (r + 1) * heads_dev] = rand_own[r]

    def first_across():
        pl.semaphore_wait(barrier, 1)
        step = jnp.where(z < half, 1, depth - 1)
        for kind, source, dest, receiver in (
            (0, k_hbm, k_pool.at[mine + 1], k_sem.at[mine]),
            (1, v_hbm, v_pool.at[mine + 1], v_sem.at[mine]),
            (2, q_hbm, q_early.at[seq * early_lanes], q_sem.at[slot]),
        ):
            remote(
                source.at[:, columns(across, x)], dest, send_sem.at[kind, step * 2 * lanes],
                receiver, device(across, x),
            ).start()
        pl.semaphore_wait(go_sem, 1)

    def all_here():
        pl.semaphore_wait(barrier, seq_count * head_count - 1)
        beside = (z == half - 2) | (z == half + 1)
        pl.when(beside)(lambda: signal(go_sem, {"seq": across, "head": head}))

    pl.when(middle)(first_across)
    pl.when(jnp.logical_not(middle))(all_here)

    steps = [depth - 1] + list(range(1, depth - 1)) + [0]

    def push(kind, source, dest, receiver, lane_steps):
        for step in steps:
            for dy in range(2):
                for dx in lane_steps:
                    if step or dy or dx:
                        there, lane = 2 * ((z + step) % depth) + (y + dy) % 2, (x + dx) % lanes
                        sender = send_sem.at[kind, (step * 2 + dy) * lanes + dx]
                        copy = remote(
                            source.at[:, columns(there, lane)], dest(dx), sender, receiver,
                            device(there, lane),
                        )
                        if dy or dx or not step:
                            copy.start()
                        else:
                            done = middle & (there == across)
                            pl.when(jnp.logical_not(done))(lambda copy=copy: copy.start())

    def post_or_keep(source, dest, sender, receiver, target, at_home):
        copy = remote(source, dest, sender, receiver, target)
        kept = pltpu.make_async_copy(source, dest, receiver)
        pl.when(at_home)(lambda: kept.start())
        pl.when(jnp.logical_not(at_home))(lambda: copy.start())

    lead = seq // heads_dev

    def owner_of(there):
        return head % 2 * heads_dev + there

    everyone = range(lanes)
    push(0, k_hbm, lambda dx: k_pool.at[mine + 1], k_sem.at[mine], everyone)
    for there in range(heads_dev):
        post_or_keep(
            rand_tile, rand_vmem.at[seq], rand_send.at[there], rand_sem.at[seq],
            {"seq": owner_of(there), "head": head}, owner_of(there) == seq,
        )
    push(
        2, q_hbm, lambda dx: q_early.at[seq * early_lanes + dx], q_sem.at[slot], range(early_lanes)
    )
    push(1, v_hbm, lambda dx: v_pool.at[mine + 1], v_sem.at[mine], everyone)
    push(
        2, q_hbm, lambda dx: q_late.at[seq * late_lanes + dx - early_lanes], q_sem.at[slot],
        range(early_lanes, lanes),
    )

    def slots(lane_steps):
        return [(s, dx, (x - dx) % lanes) for s in range(seq_count) for dx in lane_steps]

    early = slots(range(early_lanes))
    late = slots(range(early_lanes, lanes))

    def pass_on(kind, pool, sems):
        arrivals = [
            (2 * ((z - step) % depth) + (y + dy) % 2, (x - dx) % lanes)
            for step in steps[::-1]
            for dy in range(2)
            for dx in everyone
        ]
        for place, (s, lane) in enumerate(arrivals):
            block = 2 * (s * lanes + lane) + core
            piece = pool.at[block + 1]
            arrive(piece, sems.at[block])
            remote(piece, piece, pass_sem.at[kind, place], sems.at[block], partner).start()

    def collect(pool, sems):
        for n in range(span):
            block = 2 * n + 1 - core
            arrive(pool.at[block + 1], sems.at[block])

    pass_on(0, k_pool, k_sem)
    shared = remote(rand_vmem, rand_vmem, rand_send.at[heads_dev], rand_sem.at[seq_count], partner)

    def share_names():
        for s in range(seq_count):
            arrive(rand_vmem.at[s], rand_sem.at[s])
        shared.start()

    pl.when(core == lead)(share_names)
    pl.when(core != lead)(lambda: shared.wait_recv())
    names = pltpu.make_async_copy(rand_vmem, rand_smem, local_sem.at[1])
    names.start()
    for s, dx, lane in early:
        arrive(q_early.at[s * early_lanes + dx], q_sem.at[s * lanes + lane])
    collect(k_pool, k_sem)
    names.wait()

    def key_set(pool, s, lane):
        parts = [pool[pl.ds(2 * (s * lanes + lane) + core, 3)].reshape(3 * BLK, HEAD_DIM)]
        parts += [pool[glob_ref[g] + 1] for g in range(2)]
        parts += [
            pool[rand_smem[s, 2 * lane + core, r * heads_dev + column] + 1] for r in range(rand_count)
        ]
        return jnp.concatenate(parts, axis=0)

    def soften(scores):
        peaks = jnp.max(scores, axis=1, keepdims=True)
        powers = jnp.exp(scores - peaks)
        totals = jnp.sum(powers, axis=1, keepdims=True)
        return powers.astype(jnp.bfloat16), jnp.broadcast_to(totals, (totals.shape[0], HEAD_DIM))

    def scored(query, keys):
        return lax.dot_general(
            query, keys, (((1,), (1,)), ((), ())), preferred_element_type=jnp.float32
        ) * scale

    def summed(powers, values):
        return lax.dot_general(
            powers, values, (((1,), (0,)), ((), ())), preferred_element_type=jnp.float32
        )

    edge = 4 * BLK

    def sparse_scores(query, s, lane):
        scores = scored(query, key_set(k_pool, s, lane))
        near = scores[:, :edge]
        place = lax.broadcasted_iota(jnp.int32, near.shape, 1) // BLK
        block = 2 * (s * lanes + lane) + core
        outside = ((place == 0) & (block == 0)) | ((place == 2) & (block == last))
        return jnp.concatenate([jnp.where(outside, MASKED, near), scores[:, edge:]], axis=1)

    every = pl.ds(1, blocks)

    def whole(pool):
        return pool[every].reshape(blocks * BLK, HEAD_DIM)

    for n, (s, dx, lane) in enumerate(early):
        p_buf[n], tot_buf[n] = soften(
            sparse_scores(q_early[s * early_lanes + dx], s, lane)
        )
    other_seq = other // head_count
    other_step = (x - other % head_count // 2) % lanes
    last_step = (x - lanes + 1) % lanes

    def pair(pool, count, first):
        last_place = (seq_count - 1) * count + jnp.clip(last_step - first, 0, count - 1)
        other_place = other_seq * count + jnp.clip(other_step - first, 0, count - 1)
        return jnp.concatenate([pool[last_place], pool[other_place]], axis=0)

    full_p[...], full_tot[...] = soften(scored(pair(q_early, early_lanes, 0), whole(k_pool)))

    pass_on(1, v_pool, v_sem)
    collect(v_pool, v_sem)
    full_out[...] = summed(full_p[...], whole(v_pool)) / full_tot[...]

    def send(s, lane):
        n = s * lanes + lane
        rows = pl.ds(pl.multiple_of((2 * lane + core) * BLK, BLK), BLK)
        cols = pl.ds(pl.multiple_of(column * HEAD_DIM, HEAD_DIM), HEAD_DIM)
        post_or_keep(
            o_buf.at[n], out_ref.at[rows, cols], o_send.at[n], o_sem.at[column, 2 * lane + core],
            {"seq": s, "head": group}, (seq == s) & (head == group),
        )

    def finish(result, s, lane):
        block = 2 * (s * lanes + lane) + core
        result = jnp.where(last == block, full_out[:BLK], result)
        result = jnp.where(other == block, full_out[BLK:], result)
        o_buf[s * lanes + lane] = result.astype(jnp.bfloat16)

    ready = None
    for n, (s, dx, lane) in enumerate(early):
        finish(summed(p_buf[n], key_set(v_pool, s, lane)) / tot_buf[n], s, lane)
        if ready:
            send(*ready)
        ready = (s, lane)
    send(*ready)
    if late:
        for s, dx, lane in late:
            arrive(q_late.at[s * late_lanes + dx - early_lanes], q_sem.at[s * lanes + lane])
        powers, totals = soften(scored(pair(q_late, late_lanes, early_lanes), whole(k_pool)))
        full_out[...] = summed(powers, whole(v_pool)) / totals
        ready = None
        for s, dx, lane in late:
            query = q_late[s * late_lanes + dx - early_lanes]
            powers, totals = soften(sparse_scores(query, s, lane))
            finish(summed(powers, key_set(v_pool, s, lane)) / totals, s, lane)
            if ready:
                send(*ready)
            ready = (s, lane)
        send(*ready)

    tile = k_pool.at[0]
    for kind in range(3):
        for n in range(1, span):
            leave(tile, send_sem.at[kind, n])
    for kind in range(2):
        for place in range(span):
            leave(tile, pass_sem.at[kind, place])
    for there in range(heads_dev):
        pl.when(owner_of(there) != seq)(
            lambda there=there: leave(rand_tile, rand_send.at[there])
        )
    pl.when(core == lead)(lambda: shared.wait_send())
    for s, dx, lane in early + late:
        pl.when((seq != s) | (head != group))(
            lambda s=s, lane=lane: leave(tile, o_send.at[s * lanes + lane])
        )
    for col in range(heads_dev):
        for row in range(head_count):
            piece = out_ref.at[
                row * BLK : (row + 1) * BLK, col * HEAD_DIM : (col + 1) * HEAD_DIM
            ]
            arrive(piece, o_sem.at[col, row])


def headed(queries, keys, values, random_blocks, global_blocks):
    seq_count, head_count = lax.axis_size("seq"), lax.axis_size("head")
    heads_dev = queries.shape[1] // HEAD_DIM // head_count
    rand_count = random_blocks.shape[2]
    names = random_blocks.transpose(2, 0, 1)
    lanes = head_count // 2
    late_lanes = lanes // 2
    early_count, late_count = seq_count * (lanes - late_lanes), max(seq_count * late_lanes, 1)
    span = seq_count * lanes
    blocks = 2 * span
    width = (5 + rand_count) * BLK
    dma = pltpu.SemaphoreType.DMA
    tile, name_tile = (BLK, HEAD_DIM), (8, 128)

    def bf16(*shape):
        return pltpu.VMEM(shape, jnp.bfloat16)

    def f32(*shape):
        return pltpu.VMEM(shape, jnp.float32)

    result = pl.pallas_call(
        functools.partial(headed_kernel, seq_count, head_count, rand_count),
        out_shape=bf16(head_count * BLK, heads_dev * HEAD_DIM),
        in_specs=[pl.BlockSpec(memory_space=pltpu.HBM)] * 4
        + [pl.BlockSpec(memory_space=pltpu.SMEM)],
        out_specs=pl.BlockSpec(memory_space=pl.ANY),
        scratch_shapes=[
            bf16(blocks + 2, *tile),
            bf16(blocks + 2, *tile),
            bf16(early_count, *tile),
            bf16(late_count, *tile),
            pltpu.VMEM((rand_count + 1,) + names.shape[1:], jnp.int32),
            pltpu.VMEM(name_tile, jnp.int32),
            pltpu.VMEM((seq_count,) + name_tile, jnp.int32),
            pltpu.SMEM((seq_count,) + name_tile, jnp.int32),
            bf16(early_count, BLK, width),
            f32(early_count, *tile),
            bf16(2 * BLK, blocks * BLK),
            f32(2 * BLK, HEAD_DIM),
            f32(2 * BLK, HEAD_DIM),
            bf16(span, *tile),
            dma((2,)),
            pltpu.SemaphoreType.REGULAR,
            dma((3, span)),
            dma((2, span)),
            dma((heads_dev + 1,)),
            dma((span,)),
            dma((blocks,)),
            dma((blocks,)),
            dma((span,)),
            dma((heads_dev, head_count)),
            dma((seq_count + 1,)),
        ],
        compiler_params=pltpu.CompilerParams(
            collective_id=0, has_side_effects=True
        ),
    )(queries, keys, values, names, global_blocks)
    return result.astype(jnp.float32)


def shards(queries, keys, values, random_blocks, global_blocks):
    seq_count, head_count = lax.axis_size("seq"), lax.axis_size("head")
    rows, width = queries.shape
    span = seq_count * head_count // 2
    fits = 6 * rows * width * span // head_count <= POOL_LIMIT
    even = seq_count % 4 == 0 and seq_count > 4 and head_count % 2 == 0 and global_blocks.shape[0] == 2
    if fits and even and rows == BLK and width == span * HEAD_DIM:
        return headed(queries, keys, values, random_blocks, global_blocks)
    return exchanged(queries, keys, values, random_blocks, global_blocks)


def solution(mesh):
    in_specs = (
        P(("seq", "head"), None),
        P(("seq", "head"), None),
        P(("seq", "head"), None),
        P("seq", "head", None),
        P(),
    )
    out_specs = P("seq", "head")
    return jax.shard_map(shards, mesh=mesh, in_specs=in_specs, out_specs=out_specs, check_vma=False)
```
